32 devices in a mesh: enc: 4 (over z), grp: 8 (over y, x, core).
Axes of the slice: x: 2, y: 2, z: 4, core: 2. Of those that a mesh axis runs over, the one named last changes fastest.
Arguments:
- patch_feats: bfloat16 [4, 512, 8, 1152], P('enc', 'grp'), may hold values from -6 to 6
- windows: int32 [4, 512, 3, 4], P('enc', 'grp'), may hold values from 0 to 7
- counts: int32 [4, 512], P('enc', 'grp'), may hold values from 1 to 3
- owners: int32 [4, 512], P('enc', 'grp'), may hold values from 0 to 7, as said below
- norm_gain: float32 [1152], replicated, may hold values from 0.1 to 1.9
- norm_bias: float32 [1152], replicated, may hold values from -1.8 to 1.8
- proj_weight: bfloat16 [1152, 4096], replicated, may hold values from -0.1875 to 0.1875
- proj_bias: float32 [4096], replicated, may hold values from -3 to 3
Outputs:
- projected: bfloat16 [4, 1536, 4096], P('enc', 'grp')
The draws below stay inside these ranges and needn't reach their ends.
Inputs may be any that keep to these rules, and one draw needn't show every extreme that they name: `owners`: within each frame index, each aligned block of 64 clips (the clips of one device) names any section-0 rank at most 8 times, and some rank exactly 8 times.
All inputs are finite; a program needn't handle non-finite values.
Results may differ from the reference program's by a relative error of at most 0.0051.
Values may be sent and summed in bfloat16 or wider, within the bound.
A program may use at most 64 MiB of HBM per device.

```python
import jax
import jax.numpy as jnp
from jax import lax

D = 1152
DL = 4096
SAMP_DEV = 64
PSAMP = 8
SEG = 3
WIN = 4
CLIPS = 512
MOST = 8
OWN_ROWS = 192
N_ENC = 4
N_GRP = 8


def draw_owners(key, part):
    block_keys = jax.random.split(jax.random.fold_in(key, 17), N_ENC * N_GRP)

    def one_block(block_key):
        first_key, second_key = jax.random.split(block_key)
        ranking = jax.random.permutation(first_key, N_GRP)
        repeated = jnp.tile(ranking, MOST)[:SAMP_DEV]
        shuffle = jax.random.permutation(second_key, SAMP_DEV)
        return repeated[shuffle]
    blocks = jax.vmap(one_block)(block_keys)
    return blocks.reshape(N_ENC, N_GRP * SAMP_DEV).astype(jnp.int32)


def with_ends(result, stream_key, low, largest):
    extent = result.shape
    spot = [jax.random.randint(jax.random.fold_in(stream_key, axis), (), 0, extent[axis]) for axis in range(len(extent))]
    result = result.at[tuple(spot)].set(low)
    longest = extent.index(max(extent))
    spot[longest] = (spot[longest] + 1) % extent[longest]
    return result.at[tuple(spot)].set(largest)


def levels(stream_key, extent, cuts, smallest, top_value):
    loudness, own = 1.0, jax.random.fold_in(stream_key, 6)
    for axis_at, blocks in cuts:
        heights = jnp.exp(jax.random.uniform(jax.random.fold_in(own, axis_at), (blocks,), jnp.float32, smallest / len(cuts), top_value / len(cuts)))
        loudness = loudness * jnp.repeat(heights, extent[axis_at] // blocks).reshape([-1 if axis == axis_at else 1 for axis in range(len(extent))])
    return loudness


def gaussian(key, dims, scale, bound, cuts=(), dtype=jnp.bfloat16):
    drawn = scale * jax.random.normal(key, dims, jnp.float32)
    if cuts:
        drawn = drawn * levels(key, dims, cuts, -0.22, 0.18)
    return jnp.clip(drawn, -bound, bound).astype(dtype)


def setup_inputs(seed: int = 0) -> dict:
    seeds = jax.random.split(jax.random.key(seed), 9)
    patch_feats = gaussian(seeds[0], (N_ENC, CLIPS, PSAMP, D), 1.0, 6.0, ((0, 4), (1, 8)))
    windows = with_ends(jax.random.randint(seeds[1], (N_ENC, CLIPS, SEG, WIN), 0, PSAMP), jax.random.fold_in(seeds[1], 1), 0, PSAMP - 1).astype(jnp.int32)
    counts = with_ends(jax.random.randint(seeds[2], (N_ENC, CLIPS), 1, SEG + 1), jax.random.fold_in(seeds[2], 1), 1, SEG).astype(jnp.int32)
    owners = draw_owners(jax.random.fold_in(seeds[8], 71), 0)
    norm_gain = jnp.clip(1.0 + 0.18 * jax.random.normal(seeds[4], (D,), jnp.float32), 0.1, 1.9)
    norm_bias = gaussian(seeds[5], (D,), 0.3, 1.8, (), jnp.float32)
    proj_weight = gaussian(seeds[6], (D, DL), D ** -0.5, 0.1875)
    proj_bias = gaussian(seeds[7], (DL,), 0.5, 3.0, (), jnp.float32)
    return dict(patch_feats=patch_feats, windows=windows, counts=counts, owners=owners, norm_gain=norm_gain, norm_bias=norm_bias, proj_weight=proj_weight, proj_bias=proj_bias)


def pool_frame(frame_feats, frame_windows, norm_gain, norm_bias):
    values = frame_feats.astype(jnp.float32)
    average = lax.optimization_barrier(jnp.mean(values, axis=-1, keepdims=True))
    spread = lax.optimization_barrier(jnp.mean((values - average) ** 2, axis=-1, keepdims=True))
    normed = (values - average) * lax.rsqrt(spread + 1e-06) * norm_gain + norm_bias
    patch_ids = jnp.arange(PSAMP).astype(jnp.int32)
    selector = lax.optimization_barrier(jnp.sum((frame_windows[..., None] == patch_ids).astype(jnp.float32), axis=2)) / WIN
    pooled = jnp.einsum('cst,ctd->csd', selector, normed, precision=lax.Precision.HIGHEST)
    return pooled.astype(jnp.bfloat16)

def reference(patch_feats, windows, counts, owners, norm_gain, norm_bias, proj_weight, proj_bias):
    pooled = lax.map(lambda pair: pool_frame(pair[0], pair[1], norm_gain, norm_bias), (patch_feats, windows))
    following = jnp.concatenate([pooled[1:], pooled[-1:]], axis=0)
    merged = ((pooled.astype(jnp.float32) + following.astype(jnp.float32)) * 0.5).astype(jnp.bfloat16)
    rank_ids = jnp.arange(N_GRP).astype(jnp.int32)
    slot_index = jnp.arange(SEG).astype(jnp.int32)

    def place(triple):
        merged_f, counts_f, owners_f = triple
        matches = (owners_f[:, None] == rank_ids[None, :]).astype(jnp.int32)
        weighted = matches * counts_f[:, None]
        earlier = jnp.cumsum(weighted, axis=0) - weighted
        start = lax.optimization_barrier(jnp.sum(earlier * matches, axis=1)).astype(jnp.int32)
        row_index = owners_f[:, None] * OWN_ROWS + start[:, None] + slot_index[None, :]
        row_index = jnp.where(slot_index[None, :] < counts_f[:, None], row_index, N_GRP * OWN_ROWS).astype(jnp.int32)
        flat_rows = merged_f.reshape(-1, D)
        product = jnp.dot(flat_rows, proj_weight, preferred_element_type=jnp.float32) + proj_bias
        rounded = product.astype(jnp.bfloat16)
        placed = jnp.zeros((N_GRP * OWN_ROWS, DL), jnp.bfloat16)
        return placed.at[row_index.reshape(-1)].set(rounded, mode='drop')
    return lax.map(place, (merged, counts, owners))
```

```python
import functools

import jax
import jax.numpy as jnp
from jax import lax
from jax.experimental import pallas as pl
from jax.experimental.pallas import tpu as pltpu
from jax.sharding import PartitionSpec as P

MESH = pl.DeviceIdType.MESH
F32 = jnp.float32
BF16 = jnp.bfloat16


def partner(me, k, groups):
    if groups & (groups - 1):
        return (me + k) % groups
    total, bit = 0, 1
    while bit < groups:
        total = total + (me // bit + k // bit) % 2 * bit
        bit *= 2
    return total


def iota(shape, axis):
    return lax.broadcasted_iota(jnp.int32, shape, axis)


def to_column(row):
    n = row.shape[1]
    return jnp.sum(jnp.where(iota((n, n), 0) == iota((n, n), 1), row, 0.0), axis=1, keepdims=True)


def placements(count_row, owner_row, rows, slot, per_sample):
    counts, owners = count_row.astype(F32), owner_row.astype(F32)
    n = counts.shape[1]
    same = (to_column(owners) == owners) & (iota((n, n), 0) < iota((n, n), 1))
    start = jnp.sum(jnp.where(same, to_column(counts), 0.0), axis=0, keepdims=True)
    first = owners * slot + start
    row_ids = iota((rows, n), 0).astype(F32)
    return [
        (row_ids == jnp.where(counts > t, first + t, -1.0)).astype(F32).astype(BF16)
        for t in range(per_sample)
    ]


def kernel(
    groups, frames, per_sample, patches, slot,
    feats_ref, win_ref, cnt_ref, own_ref, gain_ref, bias_ref,
    packed_ref, live_ref,
    normed, pooled, zsend, zrecv, outgoing, arrived,
    all_cnt, all_own, prev_cnt, prev_own,
    z_send, z_recv, a_send, a_recv, c_send, c_recv, o_send, o_recv,
):
    frame, me = lax.axis_index("enc"), lax.axis_index("grp")
    first, last = frame == 0, frame == frames - 1
    width = feats_ref.shape[1]
    clips = cnt_ref.shape[1]
    rows = groups * slot
    order = list(range(groups - 1, -1, -1))

    barrier = pltpu.get_barrier_semaphore()
    for k in order[:-1]:
        pl.semaphore_signal(
            barrier, inc=1, device_id=(frame, partner(me, k, groups)), device_id_type=MESH
        )

    @pl.when(jnp.logical_not(first))
    def _():
        pl.semaphore_signal(barrier, inc=1, device_id=(frame - 1, me), device_id_type=MESH)

    @pl.when(jnp.logical_not(last))
    def _():
        pl.semaphore_signal(barrier, inc=1, device_id=(frame + 1, me), device_id_type=MESH)

    step_rows = 32
    gain, bias = gain_ref[...], bias_ref[...]

    def norm_step(i):
        at = pl.ds(pl.multiple_of(i * step_rows, step_rows), step_rows)
        values = feats_ref[at, :].astype(F32)
        centred = values - jnp.sum(values, axis=1, keepdims=True) * (1.0 / width)
        spread = jnp.sum(centred * centred, axis=1, keepdims=True) * (1.0 / width)
        normed[at, :] = (centred * lax.rsqrt(spread + 1e-06) * gain + bias).astype(BF16)

    steps = feats_ref.shape[0] // step_rows
    early = steps // 4
    pl.loop(0, early)(norm_step)

    neighbours = (frame + frames - 1) // frames + (2 * (frames - 1) - frame) // frames
    pl.semaphore_wait(barrier, groups - 1 + neighbours)

    def remote(src, dst, send, recv, k, device):
        return pltpu.make_async_remote_copy(
            src_ref=src, dst_ref=dst, send_sem=send.at[k], recv_sem=recv.at[k],
            device_id=device, device_id_type=MESH,
        )

    def enc_meta():
        to = (frame + 1, me)
        return (
            remote(cnt_ref, prev_cnt, c_send, c_recv, 0, to),
            remote(own_ref, prev_own, o_send, o_recv, 0, to),
        )

    def grp_meta(k):
        to = (frame, partner(me, k, groups))
        return (
            remote(cnt_ref, all_cnt.at[me], c_send, c_recv, k, to),
            remote(own_ref, all_own.at[me], o_send, o_recv, k, to),
        )

    def z_copy(k):
        o = partner(me, k, groups)
        return remote(zsend.at[o], zrecv.at[o], z_send, z_recv, k, (frame - 1, me))

    def a_copy(k):
        o = partner(me, k, groups)
        return remote(outgoing.at[o], arrived.at[me], a_send, a_recv, k, (frame, o))

    @pl.when(jnp.logical_not(last))
    def _():
        for copy in enc_meta():
            copy.start()

    for k in order[:-1]:
        for copy in grp_meta(k):
            copy.start()
    all_cnt[me] = cnt_ref[...]
    all_own[me] = own_ref[...]

    pl.loop(early, steps)(norm_step)

    cells = clips * patches
    cell_ids = iota((clips, cells), 1)
    base = iota((clips, 1), 0) * patches
    members = win_ref.shape[1]
    eye = (iota((clips, clips), 0) == iota((clips, clips), 1)).astype(F32).astype(BF16)
    for t in range(per_sample):
        picks = lax.dot_general(
            eye,
            win_ref[t].astype(F32).astype(BF16),
            (((1,), (1,)), ((), ())),
            preferred_element_type=F32,
        ).astype(jnp.int32)
        chosen = jnp.zeros((clips, cells), F32)
        for w in range(members):
            chosen += (cell_ids == base + picks[:, w : w + 1]).astype(F32)
        total = jnp.dot(chosen.astype(BF16), normed[...], preferred_element_type=F32)
        pooled[t] = (total * (1.0 / members)).astype(BF16)

    def sort_rows(count_row, owner_row):
        total = jnp.zeros((rows, width), F32)
        for t, chosen in enumerate(placements(count_row, owner_row, rows, slot, per_sample)):
            total += jnp.dot(chosen, pooled[t], preferred_element_type=F32)
        return total.astype(BF16).reshape(groups, slot, width)

    @pl.when(jnp.logical_not(first))
    def _():
        for copy in enc_meta():
            copy.wait_recv()
        zsend[...] = sort_rows(prev_cnt[...], prev_own[...])
        for k in order:
            z_copy(k).start()

    outgoing[...] = sort_rows(cnt_ref[...], own_ref[...])

    for k in order:
        o = partner(me, k, groups)

        @pl.when(jnp.logical_not(last))
        def _():
            z_copy(k).wait_recv()
            outgoing[o] = ((outgoing[o].astype(F32) + zrecv[o].astype(F32)) * 0.5).astype(BF16)

        if k:
            a_copy(k).start()
        else:
            arrived[me] = outgoing[me]

    lane = iota((1, rows), 1)
    opening, size = jnp.zeros((1, rows), F32), jnp.zeros((1, rows), F32)
    amount = jnp.zeros((1, 1), F32)
    for k in order[:-1]:
        for copy in grp_meta(k):
            copy.wait_recv()
    for s in range(groups):
        mine = all_own[s] == me
        sent = jnp.sum(jnp.where(mine, all_cnt[s], 0).astype(F32), axis=1, keepdims=True)
        opening += jnp.where(lane // slot > s, sent, 0.0)
        size += jnp.where(lane // slot == s, sent, 0.0)
        amount += sent
    within = (lane % slot).astype(F32)
    target = jnp.where(within < size, opening + within, -1.0)
    rows_out = packed_ref.shape[0]
    chosen = (iota((rows_out, rows), 0).astype(F32) == target).astype(F32).astype(BF16)
    live_ref[...] = (iota((rows_out, 1), 0).astype(F32) < amount).astype(F32)

    for k in order[:-1]:
        a_copy(k).wait_recv()
    packed_ref[...] = jnp.dot(
        chosen, arrived[...].reshape(rows, width), preferred_element_type=F32
    ).astype(BF16)

    for k in order[:-1]:
        a_copy(k).wait_send()
        for copy in grp_meta(k):
            copy.wait_send()

    @pl.when(jnp.logical_not(first))
    def _():
        for k in order:
            z_copy(k).wait_send()

    @pl.when(jnp.logical_not(last))
    def _():
        for copy in enc_meta():
            copy.wait_send()


def shards(patch_feats, windows, counts, owners, norm_gain, norm_bias, proj_weight, proj_bias):
    groups, frames = lax.axis_size("grp"), lax.axis_size("enc")
    _, clips, patches, width = patch_feats.shape
    per_sample = windows.shape[2]
    slot_rows = -(-clips // groups) * per_sample
    slot = -(-slot_rows // 8) * 8
    rows_out = groups * slot_rows
    block = (groups, slot, width)
    dma = pltpu.SemaphoreType.DMA((groups,))
    packed, live = pl.pallas_call(
        functools.partial(kernel, groups, frames, per_sample, patches, slot),
        out_shape=(
            jax.ShapeDtypeStruct((rows_out, width), BF16),
            jax.ShapeDtypeStruct((rows_out, 1), F32),
        ),
        in_specs=[pl.BlockSpec(memory_space=pltpu.VMEM)] * 6,
        out_specs=[pl.BlockSpec(memory_space=pltpu.VMEM)] * 2,
        scratch_shapes=[
            pltpu.VMEM((clips * patches, width), BF16),
            pltpu.VMEM((per_sample, clips, width), BF16),
            pltpu.VMEM(block, BF16),
            pltpu.VMEM(block, BF16),
            pltpu.VMEM(block, BF16),
            pltpu.VMEM(block, BF16),
            pltpu.VMEM((groups, 1, clips), jnp.int32),
            pltpu.VMEM((groups, 1, clips), jnp.int32),
            pltpu.VMEM((1, clips), jnp.int32),
            pltpu.VMEM((1, clips), jnp.int32),
        ]
        + [dma] * 8,
        compiler_params=pltpu.CompilerParams(
            collective_id=0, has_side_effects=True, vmem_limit_bytes=24 * 1024 * 1024
        ),
        cost_estimate=pl.CostEstimate(
            flops=10**9, bytes_accessed=20 * 10**6, transcendentals=0
        ),
    )(
        patch_feats.reshape(clips * patches, width),
        jnp.transpose(windows[0], (1, 2, 0)),
        counts,
        owners,
        norm_gain.reshape(1, width),
        norm_bias.reshape(1, width),
    )
    product = jnp.dot(packed, proj_weight, preferred_element_type=F32)
    result = jnp.where(live > 0.0, product + proj_bias, 0.0).astype(BF16)
    return result[None]


def solution(mesh):
    placed = (
        P("enc", "grp", None, None),
        P("enc", "grp", None, None),
        P("enc", "grp"),
        P("enc", "grp"),
        P(),
        P(),
        P(),
        P(),
    )
    return jax.shard_map(
        shards, mesh=mesh, in_specs=placed, out_specs=P("enc", "grp", None), check_vma=False
    )
```

```python
import functools

import jax
import jax.numpy as jnp
from jax import lax
from jax.experimental import pallas as pl
from jax.experimental.pallas import tpu as pltpu
from jax.sharding import PartitionSpec as P

MESH = pl.DeviceIdType.MESH
F32 = jnp.float32
BF16 = jnp.bfloat16


def partner(me, k, groups):
    if groups & (groups - 1):
        return (me + k) % groups
    total, bit = 0, 1
    while bit < groups:
        total = total + (me // bit + k // bit) % 2 * bit
        bit *= 2
    return total


def iota(shape, axis):
    return lax.broadcasted_iota(jnp.int32, shape, axis)


def to_column(row):
    n = row.shape[1]
    return jnp.sum(jnp.where(iota((n, n), 0) == iota((n, n), 1), row, 0.0), axis=1, keepdims=True)


def placements(count_row, owner_row, rows, slot, per_sample):
    counts, owners = count_row.astype(F32), owner_row.astype(F32)
    n = counts.shape[1]
    same = (to_column(owners) == owners) & (iota((n, n), 0) < iota((n, n), 1))
    start = jnp.sum(jnp.where(same, to_column(counts), 0.0), axis=0, keepdims=True)
    first = owners * slot + start
    row_ids = iota((rows, n), 0).astype(F32)
    return [
        (row_ids == jnp.where(counts > t, first + t, -1.0)).astype(F32).astype(BF16)
        for t in range(per_sample)
    ]


def kernel(
    groups, frames, per_sample, patches, slot,
    feats_hbm, win_hbm, cnt_hbm, own_hbm, gain_hbm, bias_hbm, weight_hbm,
    packed_ref, live_ref, weight_ref,
    feats_ref, win_ref, cnt_ref, own_ref, gain_ref, bias_ref, in_sem, feats_sem,
    normed, pooled, zsend, zrecv, outgoing, arrived,
    all_cnt, all_own, prev_cnt, prev_own,
    z_send, z_recv, a_send, a_recv, c_send, c_recv, o_send, o_recv,
):
    frame, me = lax.axis_index("enc"), lax.axis_index("grp")
    first, last = frame == 0, frame == frames - 1
    width = feats_ref.shape[1]
    clips = cnt_ref.shape[1]
    rows = groups * slot
    order = list(range(groups - 1, -1, -1))

    barrier = pltpu.get_barrier_semaphore()
    for k in order[:-1]:
        pl.semaphore_signal(
            barrier, inc=1, device_id=(frame, partner(me, k, groups)), device_id_type=MESH
        )

    @pl.when(jnp.logical_not(first))
    def _():
        pl.semaphore_signal(barrier, inc=1, device_id=(frame - 1, me), device_id_type=MESH)

    @pl.when(jnp.logical_not(last))
    def _():
        pl.semaphore_signal(barrier, inc=1, device_id=(frame + 1, me), device_id_type=MESH)

    step_rows = 32
    pieces = 4
    piece = feats_ref.shape[0] // pieces

    def feats_copy(i):
        at = pl.ds(i * piece, piece)
        return pltpu.make_async_copy(feats_hbm.at[at, :], feats_ref.at[at, :], feats_sem.at[i])

    small = [
        pltpu.make_async_copy(src, dst, in_sem.at[i])
        for i, (src, dst) in enumerate(
            (
                (cnt_hbm, cnt_ref),
                (own_hbm, own_ref),
                (gain_hbm, gain_ref),
                (bias_hbm, bias_ref),
                (win_hbm, win_ref),
                (weight_hbm, weight_ref),
            )
        )
    ]
    for copy in small[:-1]:
        copy.start()
    for i in range(pieces):
        feats_copy(i).start()
    small[-1].start()

    def norm_rows(i):
        at = pl.ds(pl.multiple_of(i * step_rows, step_rows), step_rows)
        values = feats_ref[at, :].astype(F32)
        centred = values - jnp.sum(values, axis=1, keepdims=True) * (1.0 / width)
        spread = jnp.sum(centred * centred, axis=1, keepdims=True) * (1.0 / width)
        normed[at, :] = (
            centred * lax.rsqrt(spread + 1e-06) * gain_ref[...].reshape(1, width)
            + bias_ref[...].reshape(1, width)
        ).astype(BF16)

    def norm_piece(i):
        feats_copy(i).wait()
        per = piece // step_rows
        pl.loop(i * per, (i + 1) * per, unroll=2)(norm_rows)

    for copy in small[:4]:
        copy.wait()
    neighbours = (frame + frames - 1) // frames + (2 * (frames - 1) - frame) // frames
    pl.semaphore_wait(barrier, groups - 1 + neighbours)

    def remote(src, dst, send, recv, k, device):
        return pltpu.make_async_remote_copy(
            src_ref=src, dst_ref=dst, send_sem=send.at[k], recv_sem=recv.at[k],
            device_id=device, device_id_type=MESH,
        )

    def enc_meta():
        to = (frame + 1, me)
        return (
            remote(cnt_ref, prev_cnt, c_send, c_recv, 0, to),
            remote(own_ref, prev_own, o_send, o_recv, 0, to),
        )

    def grp_meta(k):
        to = (frame, partner(me, k, groups))
        return (
            remote(cnt_ref, all_cnt.at[me], c_send, c_recv, k, to),
            remote(own_ref, all_own.at[me], o_send, o_recv, k, to),
        )

    def z_copy(k):
        o = partner(me, k, groups)
        return remote(zsend.at[o], zrecv.at[o], z_send, z_recv, k, (frame - 1, me))

    def a_copy(k):
        o = partner(me, k, groups)
        return remote(outgoing.at[o], arrived.at[me], a_send, a_recv, k, (frame, o))

    @pl.when(jnp.logical_not(last))
    def _():
        for copy in enc_meta():
            copy.start()

    for k in order[:-1]:
        for copy in grp_meta(k):
            copy.start()
    all_cnt[me] = cnt_ref[...]
    all_own[me] = own_ref[...]

    for i in range(pieces):
        norm_piece(i)
    small[4].wait()

    cells = clips * patches
    cell_ids = iota((clips, cells), 1)
    base = iota((clips, 1), 0) * patches
    members = win_ref.shape[1]
    eye = (iota((clips, clips), 0) == iota((clips, clips), 1)).astype(F32).astype(BF16)
    for t in range(per_sample):
        picks = lax.dot_general(
            eye,
            win_ref[t].astype(F32).astype(BF16),
            (((1,), (1,)), ((), ())),
            preferred_element_type=F32,
        ).astype(jnp.int32)
        chosen = jnp.zeros((clips, cells), F32)
        for w in range(members):
            chosen += (cell_ids == base + picks[:, w : w + 1]).astype(F32)
        total = jnp.dot(chosen.astype(BF16), normed[...], preferred_element_type=F32)
        pooled[t] = (total * (1.0 / members)).astype(BF16)

    def sort_rows(count_row, owner_row):
        total = jnp.zeros((rows, width), F32)
        for t, chosen in enumerate(placements(count_row, owner_row, rows, slot, per_sample)):
            total += jnp.dot(chosen, pooled[t], preferred_element_type=F32)
        return total.astype(BF16).reshape(groups, slot, width)

    @pl.when(jnp.logical_not(first))
    def _():
        for copy in enc_meta():
            copy.wait_recv()
        zsend[...] = sort_rows(prev_cnt[...], prev_own[...])
        for k in order:
            z_copy(k).start()

    outgoing[...] = sort_rows(cnt_ref[...], own_ref[...])

    for k in order:
        o = partner(me, k, groups)

        @pl.when(jnp.logical_not(last))
        def _():
            z_copy(k).wait_recv()
            outgoing[o] = ((outgoing[o].astype(F32) + zrecv[o].astype(F32)) * 0.5).astype(BF16)

        if k:
            a_copy(k).start()
        else:
            arrived[me] = outgoing[me]

    lane = iota((1, rows), 1)
    opening, size = jnp.zeros((1, rows), F32), jnp.zeros((1, rows), F32)
    amount = jnp.zeros((1, 1), F32)
    for k in order[:-1]:
        for copy in grp_meta(k):
            copy.wait_recv()
    for s in range(groups):
        mine = all_own[s] == me
        sent = jnp.sum(jnp.where(mine, all_cnt[s], 0).astype(F32), axis=1, keepdims=True)
        opening += jnp.where(lane // slot > s, sent, 0.0)
        size += jnp.where(lane // slot == s, sent, 0.0)
        amount += sent
    within = (lane % slot).astype(F32)
    target = jnp.where(within < size, opening + within, -1.0)
    rows_out = packed_ref.shape[0]
    chosen = (iota((rows_out, rows), 0).astype(F32) == target).astype(F32).astype(BF16)
    live_ref[...] = (iota((rows_out, 1), 0).astype(F32) < amount).astype(F32)

    for k in order[:-1]:
        a_copy(k).wait_recv()
    packed_ref[...] = jnp.dot(
        chosen, arrived[...].reshape(rows, width), preferred_element_type=F32
    ).astype(BF16)

    small[5].wait()
    for k in order[:-1]:
        a_copy(k).wait_send()
        for copy in grp_meta(k):
            copy.wait_send()

    @pl.when(jnp.logical_not(first))
    def _():
        for k in order:
            z_copy(k).wait_send()

    @pl.when(jnp.logical_not(last))
    def _():
        for copy in enc_meta():
            copy.wait_send()


def shards(patch_feats, windows, counts, owners, norm_gain, norm_bias, proj_weight, proj_bias):
    groups, frames = lax.axis_size("grp"), lax.axis_size("enc")
    _, clips, patches, width = patch_feats.shape
    per_sample = windows.shape[2]
    slot_rows = -(-clips // groups) * per_sample
    slot = -(-slot_rows // 8) * 8
    rows_out = groups * slot_rows
    block = (groups, slot, width)
    dma = pltpu.SemaphoreType.DMA((groups,))
    packed, live, weight = pl.pallas_call(
        functools.partial(kernel, groups, frames, per_sample, patches, slot),
        out_shape=(
            jax.ShapeDtypeStruct((rows_out, width), BF16),
            jax.ShapeDtypeStruct((rows_out, 1), F32),
            jax.ShapeDtypeStruct(proj_weight.shape, BF16),
        ),
        in_specs=[pl.BlockSpec(memory_space=pltpu.HBM)] * 7,
        out_specs=[pl.BlockSpec(memory_space=pltpu.VMEM)] * 3,
        scratch_shapes=[
            pltpu.VMEM((clips * patches, width), BF16),
            pltpu.VMEM((per_sample, windows.shape[3], clips), jnp.int32),
            pltpu.VMEM((1, clips), jnp.int32),
            pltpu.VMEM((1, clips), jnp.int32),
            pltpu.VMEM((width,), F32),
            pltpu.VMEM((width,), F32),
            pltpu.SemaphoreType.DMA((6,)),
            pltpu.SemaphoreType.DMA((4,)),
            pltpu.VMEM((clips * patches, width), BF16),
            pltpu.VMEM((per_sample, clips, width), BF16),
            pltpu.VMEM(block, BF16),
            pltpu.VMEM(block, BF16),
            pltpu.VMEM(block, BF16),
            pltpu.VMEM(block, BF16),
            pltpu.VMEM((groups, 1, clips), jnp.int32),
            pltpu.VMEM((groups, 1, clips), jnp.int32),
            pltpu.VMEM((1, clips), jnp.int32),
            pltpu.VMEM((1, clips), jnp.int32),
        ]
        + [dma] * 8,
        compiler_params=pltpu.CompilerParams(
            collective_id=0, has_side_effects=True, vmem_limit_bytes=36 * 1024 * 1024
        ),
        cost_estimate=pl.CostEstimate(
            flops=10**9, bytes_accessed=20 * 10**6, transcendentals=0
        ),
    )(
        *(
            pltpu.with_memory_space_constraint(array, pltpu.HBM)
            for array in (
                patch_feats.reshape(clips * patches, width),
                jnp.transpose(windows[0], (1, 2, 0)),
                counts,
                owners,
                norm_gain,
                norm_bias,
                proj_weight,
            )
        )
    )
    product = jnp.dot(packed, weight, preferred_element_type=F32)
    result = jnp.where(live > 0.0, product + proj_bias, 0.0).astype(BF16)
    return result[None]


def solution(mesh):
    placed = (
        P("enc", "grp", None, None),
        P("enc", "grp", None, None),
        P("enc", "grp"),
        P("enc", "grp"),
        P(),
        P(),
        P(),
        P(),
    )
    return jax.shard_map(
        shards, mesh=mesh, in_specs=placed, out_specs=P("enc", "grp", None), check_vma=False
    )
```

```python
import functools

import jax
import jax.numpy as jnp
from jax import lax
from jax.experimental import pallas as pl
from jax.experimental.pallas import tpu as pltpu
from jax.sharding import PartitionSpec as P

MESH = pl.DeviceIdType.MESH
F32 = jnp.float32
BF16 = jnp.bfloat16


def partner(me, k, groups):
    if groups & (groups - 1):
        return (me + k) % groups
    total, bit = 0, 1
    while bit < groups:
        total = total + (me // bit + k // bit) % 2 * bit
        bit *= 2
    return total


def iota(shape, axis):
    return lax.broadcasted_iota(jnp.int32, shape, axis)


def to_column(row):
    n = row.shape[1]
    return jnp.sum(jnp.where(iota((n, n), 0) == iota((n, n), 1), row, 0.0), axis=1, keepdims=True)


def placements(count_row, owner_row, slot, per_sample):
    counts, owners = count_row.astype(F32), owner_row.astype(F32)
    n = counts.shape[1]
    same = (to_column(owners) == owners) & (iota((n, n), 0) < iota((n, n), 1))
    start = jnp.sum(jnp.where(same, to_column(counts), 0.0), axis=0, keepdims=True)
    first = owners * slot + start
    targets = [jnp.where(counts > t, first + t, -1.0) for t in range(per_sample)]
    return jnp.concatenate(targets, axis=1).astype(jnp.int32)


def kernel(
    groups, frames, per_sample, patches, slot,
    feats_hbm, win_hbm, cnt_hbm, own_hbm, gain_hbm, bias_hbm, weight_hbm,
    packed_ref, live_ref, weight_ref,
    feats_ref, win_ref, cnt_ref, own_ref, gain_ref, bias_ref, in_sem, feats_sem,
    normed, pooled, zsend, zrecv, outgoing, arrived,
    all_cnt, all_own, targets, prev_targets, gather,
    z_send, z_recv, a_send, a_recv, c_send, c_recv, o_send, o_recv,
):
    frame, me = lax.axis_index("enc"), lax.axis_index("grp")
    first, last = frame == 0, frame == frames - 1
    width = feats_ref.shape[1]
    clips = cnt_ref.shape[1]
    rows = groups * slot
    order = list(range(groups - 1, -1, -1))

    step_rows = 32
    pieces = 4
    piece = feats_ref.shape[0] // pieces

    def feats_copy(i):
        at = pl.ds(i * piece, piece)
        return pltpu.make_async_copy(feats_hbm.at[at, :], feats_ref.at[at, :], feats_sem.at[i])

    small = [
        pltpu.make_async_copy(src, dst, in_sem.at[i])
        for i, (src, dst) in enumerate(
            (
                (cnt_hbm, cnt_ref),
                (own_hbm, own_ref),
                (gain_hbm, gain_ref),
                (bias_hbm, bias_ref),
                (win_hbm, win_ref),
                (weight_hbm, weight_ref),
            )
        )
    ]
    for copy in small[:-1]:
        copy.start()
    for i in range(pieces):
        feats_copy(i).start()
    small[-1].start()

    barrier = pltpu.get_barrier_semaphore()
    for k in order[:-1]:
        pl.semaphore_signal(
            barrier, inc=1, device_id=(frame, partner(me, k, groups)), device_id_type=MESH
        )

    @pl.when(jnp.logical_not(first))
    def _():
        pl.semaphore_signal(barrier, inc=1, device_id=(frame - 1, me), device_id_type=MESH)

    @pl.when(jnp.logical_not(last))
    def _():
        pl.semaphore_signal(barrier, inc=1, device_id=(frame + 1, me), device_id_type=MESH)

    def norm_rows(i):
        at = pl.ds(pl.multiple_of(i * step_rows, step_rows), step_rows)
        values = feats_ref[at, :].astype(F32)
        centred = values - jnp.sum(values, axis=1, keepdims=True) * (1.0 / width)
        spread = jnp.sum(centred * centred, axis=1, keepdims=True) * (1.0 / width)
        normed[at, :] = (
            centred * lax.rsqrt(spread + 1e-06) * gain_ref[...].reshape(1, width)
            + bias_ref[...].reshape(1, width)
        ).astype(BF16)

    def norm_piece(i):
        feats_copy(i).wait()
        per = piece // step_rows
        pl.loop(i * per, (i + 1) * per, unroll=2)(norm_rows)

    for copy in small[:-1]:
        copy.wait()
    targets[...] = placements(cnt_ref[...], own_ref[...], slot, per_sample)

    cells = clips * patches
    members = win_ref.shape[1]
    cell_ids = iota((clips, cells), 1)
    base = iota((clips, 1), 0) * patches
    eye = (iota((clips, clips), 0) == iota((clips, clips), 1)).astype(F32).astype(BF16)
    for t in range(per_sample):
        picks = base + lax.dot_general(
            eye,
            win_ref[t].astype(F32).astype(BF16),
            (((1,), (1,)), ((), ())),
            preferred_element_type=F32,
        ).astype(jnp.int32)
        chosen = jnp.zeros((clips, cells), F32)
        for w in range(members):
            chosen += (cell_ids == picks[:, w : w + 1]).astype(F32)
        gather[t * clips : (t + 1) * clips, :] = chosen.astype(BF16)

    neighbours = (frame + frames - 1) // frames + (2 * (frames - 1) - frame) // frames
    pl.semaphore_wait(barrier, groups - 1 + neighbours)

    def remote(src, dst, send, recv, k, device):
        return pltpu.make_async_remote_copy(
            src_ref=src, dst_ref=dst, send_sem=send.at[k], recv_sem=recv.at[k],
            device_id=device, device_id_type=MESH,
        )

    def enc_meta():
        return remote(targets, prev_targets, c_send, c_recv, 0, (frame + 1, me))

    def grp_meta(k):
        to = (frame, partner(me, k, groups))
        return (
            remote(cnt_ref, all_cnt.at[me], c_send, c_recv, k, to),
            remote(own_ref, all_own.at[me], o_send, o_recv, k, to),
        )

    def z_copy(k):
        o = partner(me, k, groups)
        return remote(zsend.at[o], zrecv.at[o], z_send, z_recv, k, (frame - 1, me))

    def a_copy(k):
        o = partner(me, k, groups)
        return remote(outgoing.at[o], arrived.at[me], a_send, a_recv, k, (frame, o))

    @pl.when(jnp.logical_not(last))
    def _():
        enc_meta().start()

    for k in order[:-1]:
        for copy in grp_meta(k):
            copy.start()
    all_cnt[me] = cnt_ref[...]
    all_own[me] = own_ref[...]

    for i in range(pieces):
        norm_piece(i)
    pooled[...] = (
        jnp.dot(gather[...], normed[...], preferred_element_type=F32) * (1.0 / members)
    ).astype(BF16)

    def sort_rows(target_row):
        chosen = iota((rows, target_row.shape[1]), 0) == target_row
        total = jnp.dot(
            chosen.astype(F32).astype(BF16), pooled[...], preferred_element_type=F32
        )
        return total.astype(BF16).reshape(groups, slot, width)

    @pl.when(jnp.logical_not(first))
    def _():
        enc_meta().wait_recv()
        zsend[...] = sort_rows(prev_targets[...])
        for k in order:
            z_copy(k).start()

    outgoing[...] = sort_rows(targets[...])

    lane = iota((1, rows), 1)
    opening, size = jnp.zeros((1, rows), F32), jnp.zeros((1, rows), F32)
    amount = jnp.zeros((1, 1), F32)
    for k in order[:-1]:
        for copy in grp_meta(k):
            copy.wait_recv()
    for s in range(groups):
        mine = all_own[s] == me
        sent = jnp.sum(jnp.where(mine, all_cnt[s], 0).astype(F32), axis=1, keepdims=True)
        opening += jnp.where(lane // slot > s, sent, 0.0)
        size += jnp.where(lane // slot == s, sent, 0.0)
        amount += sent
    within = (lane % slot).astype(F32)
    target = jnp.where(within < size, opening + within, -1.0)
    rows_out = packed_ref.shape[0]
    chosen = (iota((rows_out, rows), 0).astype(F32) == target).astype(F32).astype(BF16)
    live_ref[...] = (iota((rows_out, 1), 0).astype(F32) < amount).astype(F32)

    for k in order:
        o = partner(me, k, groups)

        @pl.when(jnp.logical_not(last))
        def _():
            z_copy(k).wait_recv()
            outgoing[o] = ((outgoing[o].astype(F32) + zrecv[o].astype(F32)) * 0.5).astype(BF16)

        if k:
            a_copy(k).start()
        else:
            arrived[me] = outgoing[me]

    for k in order[:-1]:
        a_copy(k).wait_recv()
    packed_ref[...] = jnp.dot(
        chosen, arrived[...].reshape(rows, width), preferred_element_type=F32
    ).astype(BF16)

    small[5].wait()
    for k in order[:-1]:
        a_copy(k).wait_send()
        for copy in grp_meta(k):
            copy.wait_send()

    @pl.when(jnp.logical_not(first))
    def _():
        for k in order:
            z_copy(k).wait_send()

    @pl.when(jnp.logical_not(last))
    def _():
        enc_meta().wait_send()


def shards(patch_feats, windows, counts, owners, norm_gain, norm_bias, proj_weight, proj_bias):
    groups, frames = lax.axis_size("grp"), lax.axis_size("enc")
    _, clips, patches, width = patch_feats.shape
    per_sample = windows.shape[2]
    slot_rows = -(-clips // groups) * per_sample
    slot = -(-slot_rows // 8) * 8
    rows_out = groups * slot_rows
    block = (groups, slot, width)
    dma = pltpu.SemaphoreType.DMA((groups,))
    packed, live, weight = pl.pallas_call(
        functools.partial(kernel, groups, frames, per_sample, patches, slot),
        out_shape=(
            jax.ShapeDtypeStruct((rows_out, width), BF16),
            jax.ShapeDtypeStruct((rows_out, 1), F32),
            jax.ShapeDtypeStruct(proj_weight.shape, BF16),
        ),
        in_specs=[pl.BlockSpec(memory_space=pltpu.HBM)] * 7,
        out_specs=[pl.BlockSpec(memory_space=pltpu.VMEM)] * 3,
        scratch_shapes=[
            pltpu.VMEM((clips * patches, width), BF16),
            pltpu.VMEM((per_sample, windows.shape[3], clips), jnp.int32),
            pltpu.VMEM((1, clips), jnp.int32),
            pltpu.VMEM((1, clips), jnp.int32),
            pltpu.VMEM((width,), F32),
            pltpu.VMEM((width,), F32),
            pltpu.SemaphoreType.DMA((6,)),
            pltpu.SemaphoreType.DMA((4,)),
            pltpu.VMEM((clips * patches, width), BF16),
            pltpu.VMEM((per_sample * clips, width), BF16),
            pltpu.VMEM(block, BF16),
            pltpu.VMEM(block, BF16),
            pltpu.VMEM(block, BF16),
            pltpu.VMEM(block, BF16),
            pltpu.VMEM((groups, 1, clips), jnp.int32),
            pltpu.VMEM((groups, 1, clips), jnp.int32),
            pltpu.VMEM((1, per_sample * clips), jnp.int32),
            pltpu.VMEM((1, per_sample * clips), jnp.int32),
            pltpu.VMEM((per_sample * clips, clips * patches), BF16),
        ]
        + [dma] * 8,
        compiler_params=pltpu.CompilerParams(
            collective_id=0, has_side_effects=True, vmem_limit_bytes=36 * 1024 * 1024
        ),
        cost_estimate=pl.CostEstimate(
            flops=10**9, bytes_accessed=20 * 10**6, transcendentals=0
        ),
    )(
        *(
            pltpu.with_memory_space_constraint(array, pltpu.HBM)
            for array in (
                patch_feats.reshape(clips * patches, width),
                jnp.transpose(windows[0], (1, 2, 0)),
                counts,
                owners,
                norm_gain,
                norm_bias,
                proj_weight,
            )
        )
    )
    product = jnp.dot(packed, weight, preferred_element_type=F32)
    result = jnp.where(live > 0.0, product + proj_bias, 0.0).astype(BF16)
    return result[None]


def solution(mesh):
    placed = (
        P("enc", "grp", None, None),
        P("enc", "grp", None, None),
        P("enc", "grp"),
        P("enc", "grp"),
        P(),
        P(),
        P(),
        P(),
    )
    return jax.shard_map(
        shards, mesh=mesh, in_specs=placed, out_specs=P("enc", "grp", None), check_vma=False
    )
```

```python
import functools

import jax
import jax.numpy as jnp
from jax import lax
from jax.experimental import pallas as pl
from jax.experimental.pallas import tpu as pltpu
from jax.sharding import PartitionSpec as P

MESH = pl.DeviceIdType.MESH
F32 = jnp.float32
BF16 = jnp.bfloat16


def partner(me, k, groups):
    if groups & (groups - 1):
        return (me + k) % groups
    total, bit = 0, 1
    while bit < groups:
        total = total + (me // bit + k // bit) % 2 * bit
        bit *= 2
    return total


def iota(shape, axis):
    return lax.broadcasted_iota(jnp.int32, shape, axis)


def to_column(row):
    n = row.shape[1]
    return jnp.sum(jnp.where(iota((n, n), 0) == iota((n, n), 1), row, 0.0), axis=1, keepdims=True)


def placements(count_row, owner_row, slot, per_sample):
    counts, owners = count_row.astype(F32), owner_row.astype(F32)
    n = counts.shape[1]
    same = (to_column(owners) == owners) & (iota((n, n), 0) < iota((n, n), 1))
    start = jnp.sum(jnp.where(same, to_column(counts), 0.0), axis=0, keepdims=True)
    first = owners * slot + start
    targets = [jnp.where(counts > t, first + t, -1.0) for t in range(per_sample)]
    return jnp.concatenate(targets, axis=1).astype(jnp.int32)


def kernel(
    groups, frames, per_sample, patches, slot,
    feats_hbm, win_hbm, cnt_hbm, own_hbm, gain_hbm, bias_hbm, weight_hbm,
    packed_ref, live_ref, weight_ref,
    feats_ref, win_ref, cnt_ref, own_ref, gain_ref, bias_ref, in_sem, feats_sem,
    normed, pooled, zsend, zrecv, outgoing, arrived,
    all_cnt, all_own, targets, prev_targets, gather,
    z_send, z_recv, a_send, a_recv, c_send, c_recv, o_send, o_recv,
):
    frame, me = lax.axis_index("enc"), lax.axis_index("grp")
    first, last = frame == 0, frame == frames - 1
    width = feats_ref.shape[1]
    clips = cnt_ref.shape[1]
    rows = groups * slot
    order = list(range(groups - 1, -1, -1))

    step_rows = 32
    pieces = 4
    piece = feats_ref.shape[0] // pieces

    def feats_copy(i):
        at = pl.ds(i * piece, piece)
        return pltpu.make_async_copy(feats_hbm.at[at, :], feats_ref.at[at, :], feats_sem.at[i])

    small = [
        pltpu.make_async_copy(src, dst, in_sem.at[i])
        for i, (src, dst) in enumerate(
            (
                (cnt_hbm, cnt_ref),
                (own_hbm, own_ref),
                (gain_hbm, gain_ref),
                (bias_hbm, bias_ref),
                (win_hbm, win_ref),
                (weight_hbm, weight_ref),
            )
        )
    ]
    for copy in small[:-1]:
        copy.start()
    for i in range(pieces):
        feats_copy(i).start()

    barrier = pltpu.get_barrier_semaphore()
    for k in order[:-1]:
        pl.semaphore_signal(
            barrier, inc=1, device_id=(frame, partner(me, k, groups)), device_id_type=MESH
        )

    @pl.when(jnp.logical_not(first))
    def _():
        pl.semaphore_signal(barrier, inc=1, device_id=(frame - 1, me), device_id_type=MESH)

    @pl.when(jnp.logical_not(last))
    def _():
        pl.semaphore_signal(barrier, inc=1, device_id=(frame + 1, me), device_id_type=MESH)

    def norm_rows(i):
        at = pl.ds(pl.multiple_of(i * step_rows, step_rows), step_rows)
        values = feats_ref[at, :].astype(F32)
        centred = values - jnp.sum(values, axis=1, keepdims=True) * (1.0 / width)
        spread = jnp.sum(centred * centred, axis=1, keepdims=True) * (1.0 / width)
        normed[at, :] = (
            centred * lax.rsqrt(spread + 1e-06) * gain_ref[...].reshape(1, width)
            + bias_ref[...].reshape(1, width)
        ).astype(BF16)

    def norm_piece(i):
        feats_copy(i).wait()
        per = piece // step_rows
        pl.loop(i * per, (i + 1) * per, unroll=4)(norm_rows)

    for copy in small[:2]:
        copy.wait()
    targets[...] = placements(cnt_ref[...], own_ref[...], slot, per_sample)

    neighbours = (frame + frames - 1) // frames + (2 * (frames - 1) - frame) // frames
    pl.semaphore_wait(barrier, groups - 1 + neighbours)

    def remote(src, dst, send, recv, k, device):
        return pltpu.make_async_remote_copy(
            src_ref=src, dst_ref=dst, send_sem=send.at[k], recv_sem=recv.at[k],
            device_id=device, device_id_type=MESH,
        )

    def enc_meta():
        return remote(targets, prev_targets, c_send, c_recv, 0, (frame + 1, me))

    def grp_meta(k):
        to = (frame, partner(me, k, groups))
        return (
            remote(cnt_ref, all_cnt.at[me], c_send, c_recv, k, to),
            remote(own_ref, all_own.at[me], o_send, o_recv, k, to),
        )

    def z_copy(k):
        o = partner(me, k, groups)
        return remote(zsend.at[o], zrecv.at[o], z_send, z_recv, k, (frame - 1, me))

    def a_copy(k):
        o = partner(me, k, groups)
        return remote(outgoing.at[o], arrived.at[me], a_send, a_recv, k, (frame, o))

    @pl.when(jnp.logical_not(last))
    def _():
        enc_meta().start()

    for k in order[:-1]:
        for copy in grp_meta(k):
            copy.start()
    all_cnt[me] = cnt_ref[...]
    all_own[me] = own_ref[...]

    for copy in small[2:5]:
        copy.wait()
    cells = clips * patches
    members = win_ref.shape[1]
    cell_ids = iota((clips, cells), 1)
    base = iota((clips, 1), 0) * patches
    eye = (iota((clips, clips), 0) == iota((clips, clips), 1)).astype(F32).astype(BF16)
    for t in range(per_sample):
        picks = base + lax.dot_general(
            eye,
            win_ref[t].astype(F32).astype(BF16),
            (((1,), (1,)), ((), ())),
            preferred_element_type=F32,
        ).astype(jnp.int32)
        chosen = jnp.zeros((clips, cells), F32)
        for w in range(members):
            chosen += (cell_ids == picks[:, w : w + 1]).astype(F32)
        gather[t * clips : (t + 1) * clips, :] = chosen.astype(BF16)

    for i in range(pieces):
        norm_piece(i)
    small[5].start()
    pooled[...] = (
        jnp.dot(gather[...], normed[...], preferred_element_type=F32) * (1.0 / members)
    ).astype(BF16)

    def sort_rows(target_row):
        chosen = iota((rows, target_row.shape[1]), 0) == target_row
        total = jnp.dot(
            chosen.astype(F32).astype(BF16), pooled[...], preferred_element_type=F32
        )
        return total.astype(BF16).reshape(groups, slot, width)

    @pl.when(jnp.logical_not(first))
    def _():
        enc_meta().wait_recv()
        zsend[...] = sort_rows(prev_targets[...])
        for k in order:
            z_copy(k).start()

    outgoing[...] = sort_rows(targets[...])

    lane = iota((1, rows), 1)
    opening, size = jnp.zeros((1, rows), F32), jnp.zeros((1, rows), F32)
    amount = jnp.zeros((1, 1), F32)
    for k in order[:-1]:
        for copy in grp_meta(k):
            copy.wait_recv()
    for s in range(groups):
        mine = all_own[s] == me
        sent = jnp.sum(jnp.where(mine, all_cnt[s], 0).astype(F32), axis=1, keepdims=True)
        opening += jnp.where(lane // slot > s, sent, 0.0)
        size += jnp.where(lane // slot == s, sent, 0.0)
        amount += sent
    within = (lane % slot).astype(F32)
    target = jnp.where(within < size, opening + within, -1.0)
    rows_out = packed_ref.shape[0]
    chosen = (iota((rows_out, rows), 0).astype(F32) == target).astype(F32).astype(BF16)
    live_ref[...] = (iota((rows_out, 1), 0).astype(F32) < amount).astype(F32)

    for k in order:
        o = partner(me, k, groups)

        @pl.when(jnp.logical_not(last))
        def _():
            z_copy(k).wait_recv()
            outgoing[o] = ((outgoing[o].astype(F32) + zrecv[o].astype(F32)) * 0.5).astype(BF16)

        if k:
            a_copy(k).start()
        else:
            arrived[me] = outgoing[me]

    for k in order[:-1]:
        a_copy(k).wait_recv()
    packed_ref[...] = jnp.dot(
        chosen, arrived[...].reshape(rows, width), preferred_element_type=F32
    ).astype(BF16)

    small[5].wait()
    for k in order[:-1]:
        a_copy(k).wait_send()
        for copy in grp_meta(k):
            copy.wait_send()

    @pl.when(jnp.logical_not(first))
    def _():
        for k in order:
            z_copy(k).wait_send()

    @pl.when(jnp.logical_not(last))
    def _():
        enc_meta().wait_send()


def shards(patch_feats, windows, counts, owners, norm_gain, norm_bias, proj_weight, proj_bias):
    groups, frames = lax.axis_size("grp"), lax.axis_size("enc")
    _, clips, patches, width = patch_feats.shape
    per_sample = windows.shape[2]
    slot_rows = -(-clips // groups) * per_sample
    slot = -(-slot_rows // 8) * 8
    rows_out = groups * slot_rows
    block = (groups, slot, width)
    dma = pltpu.SemaphoreType.DMA((groups,))
    packed, live, weight = pl.pallas_call(
        functools.partial(kernel, groups, frames, per_sample, patches, slot),
        out_shape=(
            jax.ShapeDtypeStruct((rows_out, width), BF16),
            jax.ShapeDtypeStruct((rows_out, 1), F32),
            jax.ShapeDtypeStruct(proj_weight.shape, BF16),
        ),
        in_specs=[pl.BlockSpec(memory_space=pltpu.HBM)] * 7,
        out_specs=[pl.BlockSpec(memory_space=pltpu.VMEM)] * 3,
        scratch_shapes=[
            pltpu.VMEM((clips * patches, width), BF16),
            pltpu.VMEM((per_sample, windows.shape[3], clips), jnp.int32),
            pltpu.VMEM((1, clips), jnp.int32),
            pltpu.VMEM((1, clips), jnp.int32),
            pltpu.VMEM((width,), F32),
            pltpu.VMEM((width,), F32),
            pltpu.SemaphoreType.DMA((6,)),
            pltpu.SemaphoreType.DMA((4,)),
            pltpu.VMEM((clips * patches, width), BF16),
            pltpu.VMEM((per_sample * clips, width), BF16),
            pltpu.VMEM(block, BF16),
            pltpu.VMEM(block, BF16),
            pltpu.VMEM(block, BF16),
            pltpu.VMEM(block, BF16),
            pltpu.VMEM((groups, 1, clips), jnp.int32),
            pltpu.VMEM((groups, 1, clips), jnp.int32),
            pltpu.VMEM((1, per_sample * clips), jnp.int32),
            pltpu.VMEM((1, per_sample * clips), jnp.int32),
            pltpu.VMEM((per_sample * clips, clips * patches), BF16),
        ]
        + [dma] * 8,
        compiler_params=pltpu.CompilerParams(
            collective_id=0, has_side_effects=True, vmem_limit_bytes=36 * 1024 * 1024
        ),
        cost_estimate=pl.CostEstimate(
            flops=10**9, bytes_accessed=20 * 10**6, transcendentals=0
        ),
    )(
        *(
            pltpu.with_memory_space_constraint(array, pltpu.HBM)
            for array in (
                patch_feats.reshape(clips * patches, width),
                jnp.transpose(windows[0], (1, 2, 0)),
                counts,
                owners,
                norm_gain,
                norm_bias,
                proj_weight,
            )
        )
    )
    product = jnp.dot(packed, weight, preferred_element_type=F32)
    result = jnp.where(live > 0.0, product + proj_bias, 0.0).astype(BF16)
    return result[None]


def solution(mesh):
    placed = (
        P("enc", "grp", None, None),
        P("enc", "grp", None, None),
        P("enc", "grp"),
        P("enc", "grp"),
        P(),
        P(),
        P(),
        P(),
    )
    return jax.shard_map(
        shards, mesh=mesh, in_specs=placed, out_specs=P("enc", "grp", None), check_vma=False
    )
```
